32 devices in a mesh: seq: 8 (over y, x, core), dp: 4 (over z).
Axes of the slice: x: 2, y: 2, z: 4, core: 2. Of those that a mesh axis runs over, the one named last changes fastest.
Arguments:
- queries: bfloat16 [8, 512, 4096], P('dp', 'seq'), may hold values from -8 to 8
- unrotated_key_rows: bfloat16 [8, 512, 1024], P('dp', 'seq'), may hold values from -8 to 8
- value_projection_rows: bfloat16 [8, 512, 1024], P('dp', 'seq'), may hold values from -6 to 6
- attention_output_gradient: bfloat16 [8, 512, 4096], P('dp', 'seq'), may hold values from -16 to 16
- normed_hidden_input: bfloat16 [8, 512, 4096], P('dp', 'seq'), may hold values from -6 to 6
- adapter_down_weight: bfloat16 [4096, 64], replicated, may hold values from -0.01171875 to 0.01171875
- adapter_up_weight: bfloat16 [64, 4096], replicated, may hold values from -0.01171875 to 0.01171875
- lengths: int32 [8], P('dp'), may hold values from 256 to 512, as said below
- offsets: int32 [8], P('dp'), may hold values from 0 to 31
Outputs:
- grad_query: bfloat16 [8, 512, 4096], P('dp', 'seq')
- grad_key: bfloat16 [8, 512, 1024], P('dp', 'seq')
- grad_value: bfloat16 [8, 512, 1024], P('dp', 'seq')
- grad_down: float32 [4096, 64], P('seq')
- grad_up: float32 [64, 4096], P(None, 'seq')
The draws below stay inside these ranges and needn't reach their ends.
Inputs may be any that keep to these rules, and one draw needn't show every extreme that they name: `lengths`: in every draw at least one rollout has all 512 positions valid.
All inputs are finite; a program needn't handle non-finite values.
Results may differ from the reference program's by a relative error of at most 0.018.
The reference program's roundings to bfloat16 on the way count: a program that leaves them out, or rounds other values in their place, can miss the bound.
Values may be sent and summed in bfloat16 or wider, within the bound.
A program may use at most 64 MiB of HBM per device.

```python
import jax
import jax.numpy as jnp
from jax import lax

MODEL_WIDTH = 4096
QUERY_HEADS = 32
KVH = 8
HEAD_WIDTH = 128
ADAPTER_RANK = 64
TOK_DEV = 64
SEQ_LEN = 512
ROLLOUTS = 8


def draw_queries(key, part):
    drawn = jnp.clip(jax.random.normal(jax.random.fold_in(key, 1), (ROLLOUTS, SEQ_LEN, QUERY_HEADS, HEAD_WIDTH), jnp.float32), -8.0, 8.0)
    return drawn.reshape(ROLLOUTS, SEQ_LEN, QUERY_HEADS * HEAD_WIDTH).astype(jnp.bfloat16)


def draw_unrotated_key_rows(key, part):
    drawn = jnp.clip(jax.random.normal(jax.random.fold_in(key, 2), (ROLLOUTS, SEQ_LEN, KVH, HEAD_WIDTH), jnp.float32), -8.0, 8.0)
    return drawn.reshape(ROLLOUTS, SEQ_LEN, KVH * HEAD_WIDTH).astype(jnp.bfloat16)


def draw_lengths(key, part):
    picks = jax.random.randint(jax.random.fold_in(key, 21), (ROLLOUTS,), SEQ_LEN // 2, SEQ_LEN + 1)
    longest = jax.random.randint(jax.random.fold_in(key, 22), (), 0, ROLLOUTS)
    return jnp.where(jnp.arange(ROLLOUTS, dtype=jnp.int32) == longest, SEQ_LEN, picks).astype(jnp.int32)


def with_ends(values, stream_key, least, high):
    extent = values.shape
    spot = [jax.random.randint(jax.random.fold_in(stream_key, axis), (), 0, extent[axis]) for axis in range(len(extent))]
    values = values.at[tuple(spot)].set(least)
    longest = extent.index(max(extent))
    spot[longest] = (spot[longest] + 1) % extent[longest]
    return values.at[tuple(spot)].set(high)


def level_of(key, dims, cuts, least, top_value):
    level, own = 1.0, jax.random.fold_in(key, 6)
    for dim, parts in cuts:
        draws = jnp.exp(jax.random.uniform(jax.random.fold_in(own, dim), (parts,), jnp.float32, least / len(cuts), top_value / len(cuts)))
        level = level * jnp.repeat(draws, dims[dim] // parts).reshape([-1 if axis == dim else 1 for axis in range(len(dims))])
    return level


def noise(key, extent, spread, reach, pieces=(), held_as=jnp.bfloat16):
    values = jax.random.normal(key, extent, jnp.float32) * spread
    if len(pieces) > 0:
        values = level_of(key, extent, pieces, -0.22, 0.18) * values
    return jnp.clip(values, min=-reach, max=reach).astype(held_as)


def setup_inputs(seed: int = 0) -> dict:
    seeds = jax.random.split(jax.random.key(seed), 10)
    queries = draw_queries(jax.random.fold_in(seeds[9], 71), 0)
    unrotated_key_rows = draw_unrotated_key_rows(jax.random.fold_in(seeds[9], 71), 0)
    value_projection_rows = noise(seeds[2], (ROLLOUTS, SEQ_LEN, KVH * HEAD_WIDTH), 1.0, 6.0, ((0, 4), (1, 8)))
    attention_output_gradient = noise(seeds[3], (ROLLOUTS, SEQ_LEN, QUERY_HEADS * HEAD_WIDTH), 4.0, 16.0, ((0, 4), (1, 8)))
    normed_hidden_input = noise(seeds[4], (ROLLOUTS, SEQ_LEN, MODEL_WIDTH), 1.0, 6.0, ((0, 4), (1, 8)))
    adapter_down_weight = noise(seeds[5], (MODEL_WIDTH, ADAPTER_RANK), (MODEL_WIDTH * 64) ** -0.5, 0.01171875)
    adapter_up_weight = noise(seeds[6], (ADAPTER_RANK, QUERY_HEADS * HEAD_WIDTH), (QUERY_HEADS * HEAD_WIDTH * 64) ** -0.5, 0.01171875)
    lengths = draw_lengths(jax.random.fold_in(seeds[9], 71), 0)
    offsets = with_ends(jax.random.randint(seeds[8], (ROLLOUTS,), 0, TOK_DEV // 2), jax.random.fold_in(seeds[8], 1), 0, (TOK_DEV // 2) - 1).astype(jnp.int32)
    return {"queries": queries, "unrotated_key_rows": unrotated_key_rows, "value_projection_rows": value_projection_rows, "attention_output_gradient": attention_output_gradient, "normed_hidden_input": normed_hidden_input, "adapter_down_weight": adapter_down_weight, "adapter_up_weight": adapter_up_weight, "lengths": lengths, "offsets": offsets}


rotary_base = 500000.0


def rotary_tables(length, head_size):
    half_size = head_size // 2
    frequency = rotary_base ** (-(jnp.arange(half_size, dtype=jnp.float32) * 2.0 / head_size))
    angles = jnp.arange(length, dtype=jnp.float32)[:, None] * frequency[None, :]
    return jnp.cos(angles), jnp.sin(angles)


def rotate(fields, cosine, sine_table, direction):
    half_size = fields.shape[-1] // 2
    first_half = fields[..., :half_size]
    second_half = fields[..., half_size:]
    cos_wide = cosine[:, None, :]
    sin_wide = direction * sine_table[:, None, :]
    return jnp.concatenate([first_half * cos_wide - second_half * sin_wide, second_half * cos_wide + first_half * sin_wide], axis=-1)


def head_backward(rot_query, rot_key, value_head, grad_head, offset, block_rows):
    length = rot_query.shape[0]
    head_size = rot_query.shape[1]
    score_scale = head_size ** -0.5
    key_accum = jnp.zeros((length, head_size), jnp.float32)
    value_accum = jnp.zeros((length, head_size), jnp.float32)
    query_parts = []
    for block_index in range(length // block_rows):
        begin_row = block_index * block_rows
        end_row = begin_row + block_rows
        row_index = jnp.arange(begin_row, end_row, dtype=jnp.int32)[:, None]
        col_index = jnp.arange(end_row, dtype=jnp.int32)[None, :]
        visible = (col_index == row_index) | ((col_index >= offset) & (col_index <= row_index))
        query_block = rot_query[begin_row:end_row]
        grad_block = grad_head[begin_row:end_row]
        key_block = rot_key[:end_row]
        value_block = value_head[:end_row]
        scores = jnp.dot(query_block, key_block.T, preferred_element_type=jnp.float32) * score_scale
        row_max = jnp.max(jnp.where(visible, scores, -jnp.inf), axis=1, keepdims=True)
        weights_exp = jnp.where(visible, jnp.exp(scores - row_max), 0.0)
        probability = weights_exp / jnp.sum(weights_exp, axis=1, keepdims=True)
        prob_low = probability.astype(jnp.bfloat16)
        grad_prob = jnp.dot(grad_block, value_block.T, preferred_element_type=jnp.float32)
        row_delta = jnp.sum(probability * grad_prob, axis=1, keepdims=True)
        grad_score = (probability * (grad_prob - row_delta) * score_scale).astype(jnp.bfloat16)
        query_parts.append(jnp.dot(grad_score, key_block, preferred_element_type=jnp.float32))
        key_accum = key_accum.at[:end_row].add(jnp.dot(grad_score.T, query_block, preferred_element_type=jnp.float32))
        value_accum = value_accum.at[:end_row].add(jnp.dot(prob_low.T, grad_block, preferred_element_type=jnp.float32))
    return jnp.concatenate(query_parts, axis=0), key_accum, value_accum


def take_head(source, chosen_head):
    return lax.dynamic_index_in_dim(source, chosen_head, 1, keepdims=False)


def reference(queries, unrotated_key_rows, value_projection_rows, attention_output_gradient, normed_hidden_input, adapter_down_weight, adapter_up_weight, lengths, offsets):
    length = queries.shape[1]
    query_width = queries.shape[2]
    head_count = query_width // HEAD_WIDTH
    key_groups = unrotated_key_rows.shape[2] // HEAD_WIDTH
    group_size = head_count // key_groups
    block_rows = min(512, length)
    cosine, sine_table = rotary_tables(length, HEAD_WIDTH)
    positions = jnp.arange(length, dtype=jnp.int32)

    def one_rollout(inputs):
        query_sequence, key_sequence, value_sequence, grad_sequence, valid_length, offset = inputs
        keep_mask = (positions >= offset) & (positions < valid_length)
        grad_sequence = jnp.where(keep_mask[:, None], grad_sequence, jnp.zeros_like(grad_sequence))
        rot_query = rotate(query_sequence.reshape(length, head_count, HEAD_WIDTH).astype(jnp.float32), cosine, sine_table, 1.0).astype(jnp.bfloat16)
        rot_key = rotate(key_sequence.reshape(length, key_groups, HEAD_WIDTH).astype(jnp.float32), cosine, sine_table, 1.0).astype(jnp.bfloat16)
        value_heads = value_sequence.reshape(length, key_groups, HEAD_WIDTH)
        grad_heads = grad_sequence.reshape(length, head_count, HEAD_WIDTH)

        def one_head(head_index):
            key_index = head_index // group_size
            query_grad, key_grad, value_grad = head_backward(take_head(rot_query, head_index), take_head(rot_key, key_index), take_head(value_heads, key_index), take_head(grad_heads, head_index), offset, block_rows)
            query_grad = rotate(query_grad[:, None, :], cosine, sine_table, -1.0)[:, 0].astype(jnp.bfloat16)
            key_grad = rotate(key_grad[:, None, :], cosine, sine_table, -1.0)[:, 0].astype(jnp.bfloat16)
            return query_grad, key_grad, value_grad.astype(jnp.bfloat16)

        query_all, key_all, value_all = lax.map(one_head, jnp.arange(head_count, dtype=jnp.int32))
        rollout_query = jnp.transpose(query_all, (1, 0, 2)).reshape(length, query_width)
        key_sum = key_all.astype(jnp.float32).reshape(key_groups, group_size, length, HEAD_WIDTH).sum(axis=1).astype(jnp.bfloat16)
        value_sum = value_all.astype(jnp.float32).reshape(key_groups, group_size, length, HEAD_WIDTH).sum(axis=1).astype(jnp.bfloat16)
        rollout_key = jnp.transpose(key_sum, (1, 0, 2)).reshape(length, key_groups * HEAD_WIDTH)
        rollout_value = jnp.transpose(value_sum, (1, 0, 2)).reshape(length, key_groups * HEAD_WIDTH)
        return rollout_query, rollout_key, rollout_value

    grad_query, grad_key, grad_value = lax.map(one_rollout, (queries, unrotated_key_rows, value_projection_rows, attention_output_gradient, lengths, offsets))
    hidden_state = normed_hidden_input.reshape(-1, normed_hidden_input.shape[2])
    flattened_query = grad_query.reshape(-1, query_width)
    adapter_latent = jnp.dot(hidden_state, adapter_down_weight, preferred_element_type=jnp.float32).astype(jnp.bfloat16)
    backward_gradient = jnp.dot(flattened_query, adapter_up_weight.T, preferred_element_type=jnp.float32).astype(jnp.bfloat16)
    grad_down = jnp.dot(hidden_state.T, backward_gradient, preferred_element_type=jnp.float32)
    grad_up = jnp.dot(adapter_latent.T, flattened_query, preferred_element_type=jnp.float32)
    return grad_query, grad_key, grad_value, grad_down, grad_up
```

```python
from functools import partial

import jax
import jax.numpy as jnp
from jax import lax
from jax.experimental import pallas as pl
from jax.experimental.pallas import tpu as pltpu
from jax.sharding import PartitionSpec as P

HEAD_WIDTH = 128


rotary_base = 500000.0


def partner_2(value, axis, distance):
    mask = 2**distance
    pairs = [(source, source ^ mask) for source in range(lax.axis_size(axis))]
    return lax.ppermute(value, axis, pairs)


def rotary_tables(length, head_size):
    half_size = head_size // 2
    frequency = rotary_base ** (-(jnp.arange(half_size, dtype=jnp.float32) * 2.0 / head_size))
    angles = jnp.arange(length, dtype=jnp.float32)[:, None] * frequency[None, :]
    return (jnp.cos(angles), jnp.sin(angles))


def rotate(fields, cosine, sine_table, direction):
    half_size = fields.shape[-1] // 2
    first_half = fields[..., :half_size]
    second_half = fields[..., half_size:]
    cos_wide = cosine[:, None, :]
    sin_wide = direction * sine_table[:, None, :]
    return jnp.concatenate(
        [
            first_half * cos_wide - second_half * sin_wide,
            second_half * cos_wide + first_half * sin_wide,
        ],
        axis=-1,
    )


def contract_axes(first_operand, second_operand, first_axis, second_axis):
    return lax.dot_general(
        first_operand,
        second_operand,
        (((first_axis,), (second_axis,)), ((), ())),
        preferred_element_type=jnp.float32,
    )


def block_terms(rot_query, rot_key, value_head, grad_head, offset, begin_row, end_row, score_scale):
    row_index = jnp.arange(begin_row, end_row, dtype=jnp.int32)[:, None]
    col_index = jnp.arange(end_row, dtype=jnp.int32)[None, :]
    visible = (col_index == row_index) | (col_index >= offset) & (col_index <= row_index)
    query_block = rot_query[begin_row:end_row]
    grad_block = grad_head[begin_row:end_row]
    key_block = rot_key[:end_row]
    value_block = value_head[:end_row]
    scores = contract_axes(query_block, key_block, 1, 1) * score_scale
    row_max = jnp.max(jnp.where(visible, scores, -jnp.inf), axis=1, keepdims=True)
    row_total = jnp.sum(jnp.where(visible, jnp.exp(scores - row_max), 0.0), axis=1, keepdims=True)
    grad_prob = contract_axes(grad_block, value_block, 1, 1)
    probability = jnp.where(visible, jnp.exp(scores - row_max), 0.0) / row_total
    row_delta = jnp.sum(probability * grad_prob, axis=1, keepdims=True)
    prob_low = probability.astype(jnp.bfloat16)
    grad_score = (probability * (grad_prob - row_delta) * score_scale).astype(jnp.bfloat16)
    block_grad = jnp.dot(grad_score, key_block, preferred_element_type=jnp.float32)
    key_add = contract_axes(grad_score, query_block, 0, 0)
    value_add = contract_axes(prob_low, grad_block, 0, 0)
    return (block_grad, key_add, value_add)


def head_backward(rot_query, rot_key, value_head, grad_head, offset, block_rows):
    length = rot_query.shape[0]
    head_size = rot_query.shape[1]
    score_scale = head_size ** (-0.5)
    query_parts = []
    key_terms = []
    value_terms = []
    for block_index in range(length // block_rows):
        begin_row = block_index * block_rows
        end_row = begin_row + block_rows
        live_terms = partial(
            block_terms,
            rot_query,
            rot_key,
            value_head,
            grad_head,
            offset,
            begin_row,
            end_row,
            score_scale,
        )
        results = live_terms()
        block_grad, key_add, value_add = results
        query_parts.append(block_grad)
        key_terms.append(jnp.pad(key_add, ((0, length - end_row), (0, 0))))
        value_terms.append(jnp.pad(value_add, ((0, length - end_row), (0, 0))))
    key_accum = key_terms[0]
    value_accum = value_terms[0]
    for term_index in range(1, len(key_terms)):
        key_accum = key_accum + key_terms[term_index]
        value_accum = value_accum + value_terms[term_index]
    return (jnp.concatenate(query_parts, axis=0), key_accum, value_accum)


def arrange_rows(rows, share, part_rows, key_groups):
    rollout_count = rows.shape[0]
    split = rows.reshape(rollout_count, share, part_rows, key_groups, HEAD_WIDTH)
    return jnp.transpose(split, (0, 2, 3, 1, 4)).reshape(
        rollout_count, part_rows, key_groups * share, HEAD_WIDTH
    )


def join_group(paired, share, seq_parts, part_rows):
    my_index = lax.axis_index("seq")
    rollout_count = paired.shape[1]
    local_keys = paired.shape[3]
    joined = paired[None]
    for bit in range(share.bit_length() - 1):
        partner = partner_2(joined, "seq", bit)
        upper = my_index // (1 << bit) % 2
        joined = jnp.where(
            upper == 0,
            jnp.concatenate([joined, partner], axis=0),
            jnp.concatenate([partner, joined], axis=0),
        )
    ordered = joined.reshape(share, 2, rollout_count, seq_parts, part_rows, local_keys, HEAD_WIDTH)
    ordered = jnp.transpose(ordered, (1, 2, 3, 0, 4, 5, 6))
    return ordered.reshape(2, rollout_count, seq_parts * share * part_rows, local_keys, HEAD_WIDTH)


def reduce_group(partial_sums, share, seq_parts, part_rows):
    my_index = lax.axis_index("seq")
    rollout_count = partial_sums.shape[1]
    local_keys = partial_sums.shape[3]
    split = partial_sums.reshape(
        2, rollout_count, seq_parts, share, part_rows, local_keys, HEAD_WIDTH
    )
    split = jnp.transpose(split, (3, 0, 1, 2, 4, 5, 6))
    for bit in reversed(range(share.bit_length() - 1)):
        half = split.shape[0] // 2
        lower_half = split[:half]
        upper_half = split[half:]
        upper = my_index // (1 << bit) % 2
        keep = jnp.where(upper == 0, lower_half, upper_half)
        outgoing = jnp.where(upper == 0, upper_half, lower_half)
        split = keep + partner_2(outgoing.astype(jnp.bfloat16), "seq", bit).astype(outgoing.dtype)
    return split[0].reshape(2, rollout_count, seq_parts * part_rows, local_keys, HEAD_WIDTH)


def on_device(
    queries,
    unrotated_key_rows,
    value_projection_rows,
    attention_output_gradient,
    normed_hidden_input,
    adapter_down_weight,
    adapter_up_weight,
    lengths,
    offsets,
):
    rollout_count = queries.shape[0]
    tokens = queries.shape[1]
    seq_parts = lax.axis_size("seq")
    length = tokens * seq_parts
    query_width = queries.shape[2]
    head_count = query_width // HEAD_WIDTH
    key_groups = unrotated_key_rows.shape[2] // HEAD_WIDTH
    local_heads = head_count // seq_parts
    adapter_rank_size = adapter_down_weight.shape[1]
    share = max(1, seq_parts // key_groups)
    part_rows = tokens // share
    query_tokens = queries.reshape(rollout_count, tokens, head_count, HEAD_WIDTH)
    grad_tokens = attention_output_gradient.reshape(rollout_count, tokens, head_count, HEAD_WIDTH)
    key_arranged = arrange_rows(unrotated_key_rows, share, part_rows, key_groups)
    value_arranged = arrange_rows(value_projection_rows, share, part_rows, key_groups)
    query_heads, key_parted, value_parted, grad_heads = (
        lax.all_to_all(query_tokens, "seq", split_axis=2, concat_axis=1, tiled=True),
        lax.all_to_all(key_arranged, "seq", split_axis=2, concat_axis=1, tiled=True),
        lax.all_to_all(value_arranged, "seq", split_axis=2, concat_axis=1, tiled=True),
        lax.all_to_all(grad_tokens, "seq", split_axis=2, concat_axis=1, tiled=True),
    )
    paired = join_group(jnp.stack([key_parted, value_parted], axis=0), share, seq_parts, part_rows)
    key_heads = paired[0]
    value_heads = paired[1]
    local_keys = key_heads.shape[2]
    cosine, sine_table = rotary_tables(length, HEAD_WIDTH)
    positions = jnp.arange(length, dtype=jnp.int32)
    keep_mask = (positions[None, :] >= offsets[:, None]) & (positions[None, :] < lengths[:, None])
    grad_heads = jnp.where(keep_mask[:, :, None, None], grad_heads, jnp.zeros_like(grad_heads))
    rot_query = rotate(query_heads.astype(jnp.float32), cosine, sine_table, 1.0).astype(
        jnp.bfloat16
    )
    rot_key = rotate(key_heads.astype(jnp.float32), cosine, sine_table, 1.0).astype(jnp.bfloat16)
    block_rows = min(512, length)
    query_rolls = []
    key_rolls = []
    value_rolls = []
    for rollout_slot in range(rollout_count):
        query_list = []
        key_list = []
        value_list = []
        for head_slot in range(local_heads):
            key_slot = head_slot * local_keys // local_heads
            query_grad, key_grad, value_grad = head_backward(
                rot_query[rollout_slot, :, head_slot],
                rot_key[rollout_slot, :, key_slot],
                value_heads[rollout_slot, :, key_slot],
                grad_heads[rollout_slot, :, head_slot],
                offsets[rollout_slot],
                block_rows,
            )
            query_list.append(
                rotate(query_grad[:, None, :], cosine, sine_table, -1.0)[:, 0].astype(jnp.bfloat16)
            )
            key_list.append(
                rotate(key_grad[:, None, :], cosine, sine_table, -1.0)[:, 0].astype(jnp.bfloat16)
            )
            value_list.append(value_grad.astype(jnp.bfloat16))
        query_rolls.append(jnp.stack(query_list, axis=1))
        key_rolls.append(jnp.stack(key_list, axis=1))
        value_rolls.append(jnp.stack(value_list, axis=1))
    query_back = jnp.stack(query_rolls, axis=0)
    key_parts = jnp.stack(key_rolls, axis=0)
    value_parts = jnp.stack(value_rolls, axis=0)
    shared_heads = local_heads // local_keys
    key_local = (
        key_parts.astype(jnp.float32)
        .reshape(rollout_count, length, local_keys, shared_heads, HEAD_WIDTH)
        .sum(axis=3)
    )
    value_local = (
        value_parts.astype(jnp.float32)
        .reshape(rollout_count, length, local_keys, shared_heads, HEAD_WIDTH)
        .sum(axis=3)
    )
    summed = reduce_group(
        jnp.stack([key_local, value_local], axis=0), share, seq_parts, part_rows
    ).astype(jnp.bfloat16)
    query_result, key_result, value_result = (
        lax.all_to_all(query_back, "seq", split_axis=1, concat_axis=2, tiled=True),
        lax.all_to_all(summed[0], "seq", split_axis=1, concat_axis=2, tiled=True),
        lax.all_to_all(summed[1], "seq", split_axis=1, concat_axis=2, tiled=True),
    )
    key_total = jnp.transpose(
        key_result.reshape(rollout_count, part_rows, key_groups, share, HEAD_WIDTH), (0, 3, 1, 2, 4)
    ).reshape(rollout_count, tokens, key_groups * HEAD_WIDTH)
    value_total = jnp.transpose(
        value_result.reshape(rollout_count, part_rows, key_groups, share, HEAD_WIDTH),
        (0, 3, 1, 2, 4),
    ).reshape(rollout_count, tokens, key_groups * HEAD_WIDTH)
    flattened_query = query_result.reshape(rollout_count * tokens, query_width)
    hidden_state = normed_hidden_input.reshape(rollout_count * tokens, normed_hidden_input.shape[2])
    adapter_latent = jnp.dot(
        hidden_state, adapter_down_weight, preferred_element_type=jnp.float32
    ).astype(jnp.bfloat16)
    backward_gradient = contract_axes(flattened_query, adapter_up_weight, 1, 1).astype(jnp.bfloat16)
    joined_terms = lax.psum_scatter(
        jnp.concatenate(
            [
                contract_axes(hidden_state, backward_gradient, 0, 0),
                contract_axes(flattened_query, adapter_latent, 0, 0),
            ],
            axis=1,
        ).astype(jnp.bfloat16),
        "seq",
        scatter_dimension=0,
        tiled=True,
    ).astype(jnp.float32)
    down_local = joined_terms[:, :adapter_rank_size]
    up_local = joined_terms[:, adapter_rank_size:]
    down_sum, up_sum = (
        lax.psum(down_local.astype(jnp.bfloat16), "dp").astype(jnp.float32),
        lax.psum(up_local.astype(jnp.bfloat16), "dp").astype(jnp.float32),
    )
    return (
        flattened_query.reshape(rollout_count, tokens, query_width),
        key_total,
        value_total,
        down_sum,
        up_sum.T,
    )


CHUNKS = 4
VMEM_BUDGET = 44 * 1024 * 1024
NEG = -1e30


def nt_dot(left, right):
    return lax.dot_general(
        left, right, (((1,), (1,)), ((), ())), preferred_element_type=jnp.float32
    )


def subsets(bits):
    masks = [0]
    for bit in bits:
        masks = masks + [mask | (1 << bit) for mask in masks]
    return masks


def fused_kernel(
    n_seq,
    n_dp,
    n_roll,
    tokens,
    kv_heads,
    group,
    rank,
    chunks,
    off_ref,
    len_ref,
    cos_ref,
    sin_ref,
    q_ref,
    k_ref,
    v_ref,
    g_ref,
    hid_ref,
    down_ref,
    up_ref,
    gq_ref,
    gk_ref,
    gv_ref,
    gd_ref,
    gu_ref,
    kv_all,
    dkv,
    red_buf,
    ad_buf,
    ad_red,
    dp_buf,
    ag_send,
    ag_recv,
    rs_send,
    rs_recv,
    ad_send,
    ad_recv,
    dp_send,
    dp_recv,
):
    me = lax.axis_index("seq")
    my_dp = lax.axis_index("dp")
    n_bits = n_seq.bit_length() - 1
    chip_bits = list(range(1, n_bits))
    gather_orders = [chip_bits + [0], chip_bits[::-1] + [0]]
    reduce_orders = [[0] + chip_bits[::-1], [0] + chip_bits]
    heads_per = kv_heads // chunks
    width = HEAD_WIDTH
    rows = group * tokens
    length = n_seq * tokens
    scale = width ** (-0.5)
    cols = q_ref.shape[1] // n_seq
    pending = []

    barrier = pltpu.get_barrier_semaphore()
    for bit in range(n_bits):
        pl.semaphore_signal(barrier, inc=1, device_id={"seq": me ^ (1 << bit)})
    for step in range(1, n_dp):
        pl.semaphore_signal(barrier, inc=1, device_id={"dp": lax.rem(my_dp + step, n_dp)})

    cos = cos_ref[...]
    sin = sin_ref[...]

    def slot_rows(mask):
        return pl.ds(pl.multiple_of((me ^ mask) * tokens, tokens), tokens)

    def load_chunk(c):
        for h in range(c * heads_per, (c + 1) * heads_per):
            for r in range(n_roll):
                span = slice(r * tokens, (r + 1) * tokens)
                lane = slice(h * width, (h + 1) * width)
                key = k_ref[span, lane].astype(jnp.float32)
                key = key * cos + pltpu.roll(key, width // 2, 1) * sin
                kv_all[0, h, r, slot_rows(0), :] = key.astype(jnp.bfloat16)
                kv_all[1, h, r, slot_rows(0), :] = v_ref[span, lane]

    gather_ops = {}

    def gather_send(c, stage):
        for t in range(2):
            order = gather_orders[t]
            bit = order[stage]
            for mask in subsets(order[:stage]):
                block = kv_all.at[
                    t, pl.ds(c * heads_per, heads_per), slice(None), slot_rows(mask), slice(None)
                ]
                got = mask | (1 << bit)
                copy = pltpu.make_async_remote_copy(
                    src_ref=block,
                    dst_ref=block,
                    send_sem=ag_send.at[t, c, got],
                    recv_sem=ag_recv.at[t, c, got],
                    device_id={"seq": me ^ (1 << bit)},
                )
                copy.start()
                gather_ops.setdefault((c, stage), []).append(copy)
                pending.append(copy)

    def gather_wait(c, stage):
        for copy in gather_ops[(c, stage)]:
            copy.wait_recv()

    reduce_ops = {}

    def reduce_send(c, stage):
        for t in range(2):
            order = reduce_orders[t]
            bit = order[stage]
            for rest in subsets(order[stage + 1 :]):
                mask = rest | (1 << bit)
                head_span = pl.ds(c * heads_per, heads_per)
                copy = pltpu.make_async_remote_copy(
                    src_ref=dkv.at[t, head_span, slice(None), slot_rows(mask), slice(None)],
                    dst_ref=red_buf.at[t, mask, head_span],
                    send_sem=rs_send.at[t, c, mask],
                    recv_sem=rs_recv.at[t, c, mask],
                    device_id={"seq": me ^ (1 << bit)},
                )
                copy.start()
                reduce_ops.setdefault((c, stage), []).append((t, mask, rest, copy))
                pending.append(copy)

    def reduce_add(c, stage):
        for t, mask, rest, copy in reduce_ops[(c, stage)]:
            copy.wait_recv()
            for h in range(c * heads_per, (c + 1) * heads_per):
                for r in range(n_roll):
                    total = dkv[t, h, r, slot_rows(rest), :].astype(jnp.float32)
                    total = total + red_buf[t, mask, h, r].astype(jnp.float32)
                    if stage < n_bits - 1:
                        dkv[t, h, r, slot_rows(rest), :] = total.astype(jnp.bfloat16)
                        continue
                    span = slice(r * tokens, (r + 1) * tokens)
                    lane = slice(h * width, (h + 1) * width)
                    if t == 0:
                        total = total * cos - pltpu.roll(total, width // 2, 1) * sin
                        gk_ref[span, lane] = total.astype(jnp.bfloat16)
                    else:
                        gv_ref[span, lane] = total.astype(jnp.bfloat16)

    def advance_reduce(c, stage):
        if stage > 0:
            reduce_add(c, stage - 1)
        if stage < n_bits:
            reduce_send(c, stage)

    adapter_ops = {}

    def adapter_send(stage):
        for t in range(2):
            order = reduce_orders[t]
            bit = order[stage]
            for rest in subsets(order[stage + 1 :]):
                mask = rest | (1 << bit)
                copy = pltpu.make_async_remote_copy(
                    src_ref=ad_buf.at[t, me ^ mask],
                    dst_ref=ad_red.at[t, mask],
                    send_sem=ad_send.at[t, mask],
                    recv_sem=ad_recv.at[t, mask],
                    device_id={"seq": me ^ (1 << bit)},
                )
                copy.start()
                adapter_ops.setdefault(stage, []).append((t, mask, rest, copy))
                pending.append(copy)

    def adapter_add(stage):
        for t, mask, rest, copy in adapter_ops[stage]:
            copy.wait_recv()
            total = ad_buf[t, me ^ rest].astype(jnp.float32) + ad_red[t, mask].astype(jnp.float32)
            total = total.astype(jnp.bfloat16)
            if stage < n_bits - 1:
                ad_buf[t, me ^ rest] = total
            else:
                dp_buf[my_dp, t] = total

    def advance_adapter(stage):
        if stage > 0:
            adapter_add(stage - 1)
        if stage < n_bits:
            adapter_send(stage)

    key_index = lax.broadcasted_iota(jnp.int32, (length, rows), 0)
    row_index = me * tokens + lax.broadcasted_iota(jnp.int32, (1, rows), 1) % tokens
    token_index = me * tokens + lax.broadcasted_iota(jnp.int32, (tokens, width), 0)

    def pair_work(c, index):
        h = c * heads_per + index // n_roll
        r = index % n_roll
        span = pl.ds(pl.multiple_of(r * tokens, tokens), tokens)
        offset = off_ref[r]
        keep = (token_index >= offset) & (token_index < len_ref[r])
        queries = []
        grads = []
        for j in range(group):
            lane = pl.ds(pl.multiple_of((h * group + j) * width, width), width)
            query = q_ref[span, lane].astype(jnp.float32)
            query = query * cos + pltpu.roll(query, width // 2, 1) * sin
            queries.append(query.astype(jnp.bfloat16))
            grad = g_ref[span, lane].astype(jnp.float32)
            grads.append(jnp.where(keep, grad, 0.0).astype(jnp.bfloat16))
        query = jnp.concatenate(queries, axis=0)
        grad = jnp.concatenate(grads, axis=0)
        key = kv_all[0, h, r]
        value = kv_all[1, h, r]
        visible = (key_index == row_index) | ((key_index >= offset) & (key_index <= row_index))
        scores = jnp.where(visible, nt_dot(key, query) * scale, NEG)
        weights = jnp.exp(scores - jnp.max(scores, axis=0, keepdims=True))
        prob = weights * (1.0 / jnp.sum(weights, axis=0, keepdims=True))
        grad_prob = nt_dot(value, grad)
        delta = jnp.sum(prob * grad_prob, axis=0, keepdims=True)
        grad_score = (prob * (grad_prob - delta) * scale).astype(jnp.bfloat16)
        prob_low = prob.astype(jnp.bfloat16)
        dkv[1, h, r] = jnp.dot(prob_low, grad, preferred_element_type=jnp.float32).astype(
            jnp.bfloat16
        )
        dkv[0, h, r] = jnp.dot(grad_score, query, preferred_element_type=jnp.float32).astype(
            jnp.bfloat16
        )
        back = jnp.dot(key.T, grad_score, preferred_element_type=jnp.float32).T
        for j in range(group):
            lane = pl.ds(pl.multiple_of((h * group + j) * width, width), width)
            part = back[j * tokens : (j + 1) * tokens]
            part = part * cos - pltpu.roll(part, width // 2, 1) * sin
            gq_ref[span, lane] = part.astype(jnp.bfloat16)

    def compute_chunk(c):
        def body(index, carry):
            pair_work(c, index)
            return carry

        lax.fori_loop(0, heads_per * n_roll, body, 0)

    load_chunk(0)
    pl.semaphore_wait(barrier, n_bits + n_dp - 1)
    latent = None
    for slot in range(chunks + 2 * n_bits + 1):
        for c in range(chunks):
            stage = slot - c
            if stage == 0 and c > 0:
                load_chunk(c)
            if 0 < stage <= n_bits:
                gather_wait(c, stage - 1)
            if 0 <= stage < n_bits:
                gather_send(c, stage)
        for c in range(chunks):
            stage = slot - c - n_bits
            if 1 <= stage <= n_bits:
                advance_reduce(c, stage)
        if slot == 0:
            latent = (
                jnp.dot(hid_ref[...], down_ref[...], preferred_element_type=jnp.float32)
                .T.astype(jnp.bfloat16)
            )
        ready = slot - n_bits
        if 0 <= ready < chunks:
            compute_chunk(ready)
            advance_reduce(ready, 0)
        if ready == chunks - 1:
            back = nt_dot(up_ref[...], gq_ref[...]).astype(jnp.bfloat16)
            for d in range(n_seq):
                lane = slice(d * cols, (d + 1) * cols)
                ad_buf[0, d] = jnp.dot(
                    back, hid_ref[:, lane], preferred_element_type=jnp.float32
                ).astype(jnp.bfloat16)
                ad_buf[1, d] = jnp.dot(
                    latent, gq_ref[:, lane], preferred_element_type=jnp.float32
                ).astype(jnp.bfloat16)
            advance_adapter(0)
        elif chunks <= ready < chunks + n_bits:
            advance_adapter(ready - chunks + 1)

    dp_ops = []
    for step in range(1, n_dp):
        copy = pltpu.make_async_remote_copy(
            src_ref=dp_buf.at[my_dp],
            dst_ref=dp_buf.at[my_dp],
            send_sem=dp_send.at[step],
            recv_sem=dp_recv.at[step],
            device_id={"dp": lax.rem(my_dp + step, n_dp)},
        )
        copy.start()
        dp_ops.append(copy)
        pending.append(copy)
    for copy in dp_ops:
        copy.wait_recv()
    down_total = dp_buf[0, 0].astype(jnp.float32)
    up_total = dp_buf[0, 1].astype(jnp.float32)
    for d in range(1, n_dp):
        down_total = down_total + dp_buf[d, 0].astype(jnp.float32)
        up_total = up_total + dp_buf[d, 1].astype(jnp.float32)
    gd_ref[...] = down_total.T
    gu_ref[...] = up_total
    for copy in pending:
        copy.wait_send()


def fused_on_device(
    n_seq,
    n_dp,
    queries,
    unrotated_key_rows,
    value_projection_rows,
    attention_output_gradient,
    normed_hidden_input,
    adapter_down_weight,
    adapter_up_weight,
    lengths,
    offsets,
):
    n_roll, tokens, q_width = queries.shape
    kv_width = unrotated_key_rows.shape[2]
    kv_heads = kv_width // HEAD_WIDTH
    group = q_width // kv_width
    rank = adapter_down_weight.shape[1]
    chunks = min(CHUNKS, kv_heads)
    flat = n_roll * tokens
    half = HEAD_WIDTH // 2
    frequency = rotary_base ** (-(jnp.arange(half, dtype=jnp.float32) * 2.0 / HEAD_WIDTH))
    positions = lax.axis_index("seq") * tokens + jnp.arange(tokens, dtype=jnp.int32)
    angles = positions.astype(jnp.float32)[:, None] * frequency[None, :]
    cosine, sine = jnp.cos(angles), jnp.sin(angles)
    cos_wide = jnp.concatenate([cosine, cosine], axis=1)
    sin_wide = jnp.concatenate([-sine, sine], axis=1)
    vmem = pl.BlockSpec(memory_space=pltpu.VMEM)
    smem = pl.BlockSpec(memory_space=pltpu.SMEM)
    cols = q_width // n_seq
    low = jnp.bfloat16
    dma = pltpu.SemaphoreType.DMA
    outs = pl.pallas_call(
        partial(fused_kernel, n_seq, n_dp, n_roll, tokens, kv_heads, group, rank, chunks),
        out_shape=(
            jax.ShapeDtypeStruct((flat, q_width), low),
            jax.ShapeDtypeStruct((flat, kv_width), low),
            jax.ShapeDtypeStruct((flat, kv_width), low),
            jax.ShapeDtypeStruct((cols, rank), jnp.float32),
            jax.ShapeDtypeStruct((rank, cols), jnp.float32),
        ),
        in_specs=[smem, smem] + [vmem] * 9,
        out_specs=[vmem] * 5,
        scratch_shapes=[
            pltpu.VMEM((2, kv_heads, n_roll, n_seq * tokens, HEAD_WIDTH), low),
            pltpu.VMEM((2, kv_heads, n_roll, n_seq * tokens, HEAD_WIDTH), low),
            pltpu.VMEM((2, n_seq, kv_heads, n_roll, tokens, HEAD_WIDTH), low),
            pltpu.VMEM((2, n_seq, rank, cols), low),
            pltpu.VMEM((2, n_seq, rank, cols), low),
            pltpu.VMEM((n_dp, 2, rank, cols), low),
            dma((2, chunks, n_seq)),
            dma((2, chunks, n_seq)),
            dma((2, chunks, n_seq)),
            dma((2, chunks, n_seq)),
            dma((2, n_seq)),
            dma((2, n_seq)),
            dma((n_dp,)),
            dma((n_dp,)),
        ],
        compiler_params=pltpu.CompilerParams(
            collective_id=0, has_side_effects=True, vmem_limit_bytes=60 * 1024 * 1024
        ),
    )(
        offsets,
        lengths,
        cos_wide,
        sin_wide,
        queries.reshape(flat, q_width),
        unrotated_key_rows.reshape(flat, kv_width),
        value_projection_rows.reshape(flat, kv_width),
        attention_output_gradient.reshape(flat, q_width),
        normed_hidden_input.reshape(flat, q_width),
        adapter_down_weight,
        adapter_up_weight,
    )
    grad_query, grad_key, grad_value, grad_down, grad_up = outs
    return (
        grad_query.reshape(n_roll, tokens, q_width),
        grad_key.reshape(n_roll, tokens, kv_width),
        grad_value.reshape(n_roll, tokens, kv_width),
        grad_down,
        grad_up,
    )


def dispatch(mesh, *args):
    n_seq = mesh.shape["seq"]
    n_roll, tokens, q_width = args[0].shape
    kv_width = args[1].shape[2]
    gathered = 2 * n_roll * n_seq * tokens * kv_width * 2
    if 3 * gathered + 7 * n_roll * tokens * q_width * 2 > VMEM_BUDGET:
        return on_device(*args)
    return fused_on_device(n_seq, mesh.shape["dp"], *args)


def solution(mesh):
    in_specs = (
        P("dp", "seq", None),
        P("dp", "seq", None),
        P("dp", "seq", None),
        P("dp", "seq", None),
        P("dp", "seq", None),
        P(),
        P(),
        P("dp"),
        P("dp"),
    )
    out_specs = (
        P("dp", "seq", None),
        P("dp", "seq", None),
        P("dp", "seq", None),
        P("seq", None),
        P(None, "seq"),
    )
    return jax.shard_map(
        partial(dispatch, mesh), mesh=mesh, in_specs=in_specs, out_specs=out_specs, check_vma=False
    )
```

```python
from functools import partial

import jax
import jax.numpy as jnp
from jax import lax
from jax.experimental import pallas as pl
from jax.experimental.pallas import tpu as pltpu
from jax.sharding import PartitionSpec as P

HEAD_WIDTH = 128


rotary_base = 500000.0


def partner_2(value, axis, distance):
    mask = 2**distance
    pairs = [(source, source ^ mask) for source in range(lax.axis_size(axis))]
    return lax.ppermute(value, axis, pairs)


def rotary_tables(length, head_size):
    half_size = head_size // 2
    frequency = rotary_base ** (-(jnp.arange(half_size, dtype=jnp.float32) * 2.0 / head_size))
    angles = jnp.arange(length, dtype=jnp.float32)[:, None] * frequency[None, :]
    return (jnp.cos(angles), jnp.sin(angles))


def rotate(fields, cosine, sine_table, direction):
    half_size = fields.shape[-1] // 2
    first_half = fields[..., :half_size]
    second_half = fields[..., half_size:]
    cos_wide = cosine[:, None, :]
    sin_wide = direction * sine_table[:, None, :]
    return jnp.concatenate(
        [
            first_half * cos_wide - second_half * sin_wide,
            second_half * cos_wide + first_half * sin_wide,
        ],
        axis=-1,
    )


def contract_axes(first_operand, second_operand, first_axis, second_axis):
    return lax.dot_general(
        first_operand,
        second_operand,
        (((first_axis,), (second_axis,)), ((), ())),
        preferred_element_type=jnp.float32,
    )


def block_terms(rot_query, rot_key, value_head, grad_head, offset, begin_row, end_row, score_scale):
    row_index = jnp.arange(begin_row, end_row, dtype=jnp.int32)[:, None]
    col_index = jnp.arange(end_row, dtype=jnp.int32)[None, :]
    visible = (col_index == row_index) | (col_index >= offset) & (col_index <= row_index)
    query_block = rot_query[begin_row:end_row]
    grad_block = grad_head[begin_row:end_row]
    key_block = rot_key[:end_row]
    value_block = value_head[:end_row]
    scores = contract_axes(query_block, key_block, 1, 1) * score_scale
    row_max = jnp.max(jnp.where(visible, scores, -jnp.inf), axis=1, keepdims=True)
    row_total = jnp.sum(jnp.where(visible, jnp.exp(scores - row_max), 0.0), axis=1, keepdims=True)
    grad_prob = contract_axes(grad_block, value_block, 1, 1)
    probability = jnp.where(visible, jnp.exp(scores - row_max), 0.0) / row_total
    row_delta = jnp.sum(probability * grad_prob, axis=1, keepdims=True)
    prob_low = probability.astype(jnp.bfloat16)
    grad_score = (probability * (grad_prob - row_delta) * score_scale).astype(jnp.bfloat16)
    block_grad = jnp.dot(grad_score, key_block, preferred_element_type=jnp.float32)
    key_add = contract_axes(grad_score, query_block, 0, 0)
    value_add = contract_axes(prob_low, grad_block, 0, 0)
    return (block_grad, key_add, value_add)


def head_backward(rot_query, rot_key, value_head, grad_head, offset, block_rows):
    length = rot_query.shape[0]
    head_size = rot_query.shape[1]
    score_scale = head_size ** (-0.5)
    query_parts = []
    key_terms = []
    value_terms = []
    for block_index in range(length // block_rows):
        begin_row = block_index * block_rows
        end_row = begin_row + block_rows
        live_terms = partial(
            block_terms,
            rot_query,
            rot_key,
            value_head,
            grad_head,
            offset,
            begin_row,
            end_row,
            score_scale,
        )
        results = live_terms()
        block_grad, key_add, value_add = results
        query_parts.append(block_grad)
        key_terms.append(jnp.pad(key_add, ((0, length - end_row), (0, 0))))
        value_terms.append(jnp.pad(value_add, ((0, length - end_row), (0, 0))))
    key_accum = key_terms[0]
    value_accum = value_terms[0]
    for term_index in range(1, len(key_terms)):
        key_accum = key_accum + key_terms[term_index]
        value_accum = value_accum + value_terms[term_index]
    return (jnp.concatenate(query_parts, axis=0), key_accum, value_accum)


def arrange_rows(rows, share, part_rows, key_groups):
    rollout_count = rows.shape[0]
    split = rows.reshape(rollout_count, share, part_rows, key_groups, HEAD_WIDTH)
    return jnp.transpose(split, (0, 2, 3, 1, 4)).reshape(
        rollout_count, part_rows, key_groups * share, HEAD_WIDTH
    )


def join_group(paired, share, seq_parts, part_rows):
    my_index = lax.axis_index("seq")
    rollout_count = paired.shape[1]
    local_keys = paired.shape[3]
    joined = paired[None]
    for bit in range(share.bit_length() - 1):
        partner = partner_2(joined, "seq", bit)
        upper = my_index // (1 << bit) % 2
        joined = jnp.where(
            upper == 0,
            jnp.concatenate([joined, partner], axis=0),
            jnp.concatenate([partner, joined], axis=0),
        )
    ordered = joined.reshape(share, 2, rollout_count, seq_parts, part_rows, local_keys, HEAD_WIDTH)
    ordered = jnp.transpose(ordered, (1, 2, 3, 0, 4, 5, 6))
    return ordered.reshape(2, rollout_count, seq_parts * share * part_rows, local_keys, HEAD_WIDTH)


def reduce_group(partial_sums, share, seq_parts, part_rows):
    my_index = lax.axis_index("seq")
    rollout_count = partial_sums.shape[1]
    local_keys = partial_sums.shape[3]
    split = partial_sums.reshape(
        2, rollout_count, seq_parts, share, part_rows, local_keys, HEAD_WIDTH
    )
    split = jnp.transpose(split, (3, 0, 1, 2, 4, 5, 6))
    for bit in reversed(range(share.bit_length() - 1)):
        half = split.shape[0] // 2
        lower_half = split[:half]
        upper_half = split[half:]
        upper = my_index // (1 << bit) % 2
        keep = jnp.where(upper == 0, lower_half, upper_half)
        outgoing = jnp.where(upper == 0, upper_half, lower_half)
        split = keep + partner_2(outgoing.astype(jnp.bfloat16), "seq", bit).astype(outgoing.dtype)
    return split[0].reshape(2, rollout_count, seq_parts * part_rows, local_keys, HEAD_WIDTH)


def on_device(
    queries,
    unrotated_key_rows,
    value_projection_rows,
    attention_output_gradient,
    normed_hidden_input,
    adapter_down_weight,
    adapter_up_weight,
    lengths,
    offsets,
):
    rollout_count = queries.shape[0]
    tokens = queries.shape[1]
    seq_parts = lax.axis_size("seq")
    length = tokens * seq_parts
    query_width = queries.shape[2]
    head_count = query_width // HEAD_WIDTH
    key_groups = unrotated_key_rows.shape[2] // HEAD_WIDTH
    local_heads = head_count // seq_parts
    adapter_rank_size = adapter_down_weight.shape[1]
    share = max(1, seq_parts // key_groups)
    part_rows = tokens // share
    query_tokens = queries.reshape(rollout_count, tokens, head_count, HEAD_WIDTH)
    grad_tokens = attention_output_gradient.reshape(rollout_count, tokens, head_count, HEAD_WIDTH)
    key_arranged = arrange_rows(unrotated_key_rows, share, part_rows, key_groups)
    value_arranged = arrange_rows(value_projection_rows, share, part_rows, key_groups)
    query_heads, key_parted, value_parted, grad_heads = (
        lax.all_to_all(query_tokens, "seq", split_axis=2, concat_axis=1, tiled=True),
        lax.all_to_all(key_arranged, "seq", split_axis=2, concat_axis=1, tiled=True),
        lax.all_to_all(value_arranged, "seq", split_axis=2, concat_axis=1, tiled=True),
        lax.all_to_all(grad_tokens, "seq", split_axis=2, concat_axis=1, tiled=True),
    )
    paired = join_group(jnp.stack([key_parted, value_parted], axis=0), share, seq_parts, part_rows)
    key_heads = paired[0]
    value_heads = paired[1]
    local_keys = key_heads.shape[2]
    cosine, sine_table = rotary_tables(length, HEAD_WIDTH)
    positions = jnp.arange(length, dtype=jnp.int32)
    keep_mask = (positions[None, :] >= offsets[:, None]) & (positions[None, :] < lengths[:, None])
    grad_heads = jnp.where(keep_mask[:, :, None, None], grad_heads, jnp.zeros_like(grad_heads))
    rot_query = rotate(query_heads.astype(jnp.float32), cosine, sine_table, 1.0).astype(
        jnp.bfloat16
    )
    rot_key = rotate(key_heads.astype(jnp.float32), cosine, sine_table, 1.0).astype(jnp.bfloat16)
    block_rows = min(512, length)
    query_rolls = []
    key_rolls = []
    value_rolls = []
    for rollout_slot in range(rollout_count):
        query_list = []
        key_list = []
        value_list = []
        for head_slot in range(local_heads):
            key_slot = head_slot * local_keys // local_heads
            query_grad, key_grad, value_grad = head_backward(
                rot_query[rollout_slot, :, head_slot],
                rot_key[rollout_slot, :, key_slot],
                value_heads[rollout_slot, :, key_slot],
                grad_heads[rollout_slot, :, head_slot],
                offsets[rollout_slot],
                block_rows,
            )
            query_list.append(
                rotate(query_grad[:, None, :], cosine, sine_table, -1.0)[:, 0].astype(jnp.bfloat16)
            )
            key_list.append(
                rotate(key_grad[:, None, :], cosine, sine_table, -1.0)[:, 0].astype(jnp.bfloat16)
            )
            value_list.append(value_grad.astype(jnp.bfloat16))
        query_rolls.append(jnp.stack(query_list, axis=1))
        key_rolls.append(jnp.stack(key_list, axis=1))
        value_rolls.append(jnp.stack(value_list, axis=1))
    query_back = jnp.stack(query_rolls, axis=0)
    key_parts = jnp.stack(key_rolls, axis=0)
    value_parts = jnp.stack(value_rolls, axis=0)
    shared_heads = local_heads // local_keys
    key_local = (
        key_parts.astype(jnp.float32)
        .reshape(rollout_count, length, local_keys, shared_heads, HEAD_WIDTH)
        .sum(axis=3)
    )
    value_local = (
        value_parts.astype(jnp.float32)
        .reshape(rollout_count, length, local_keys, shared_heads, HEAD_WIDTH)
        .sum(axis=3)
    )
    summed = reduce_group(
        jnp.stack([key_local, value_local], axis=0), share, seq_parts, part_rows
    ).astype(jnp.bfloat16)
    query_result, key_result, value_result = (
        lax.all_to_all(query_back, "seq", split_axis=1, concat_axis=2, tiled=True),
        lax.all_to_all(summed[0], "seq", split_axis=1, concat_axis=2, tiled=True),
        lax.all_to_all(summed[1], "seq", split_axis=1, concat_axis=2, tiled=True),
    )
    key_total = jnp.transpose(
        key_result.reshape(rollout_count, part_rows, key_groups, share, HEAD_WIDTH), (0, 3, 1, 2, 4)
    ).reshape(rollout_count, tokens, key_groups * HEAD_WIDTH)
    value_total = jnp.transpose(
        value_result.reshape(rollout_count, part_rows, key_groups, share, HEAD_WIDTH),
        (0, 3, 1, 2, 4),
    ).reshape(rollout_count, tokens, key_groups * HEAD_WIDTH)
    flattened_query = query_result.reshape(rollout_count * tokens, query_width)
    hidden_state = normed_hidden_input.reshape(rollout_count * tokens, normed_hidden_input.shape[2])
    adapter_latent = jnp.dot(
        hidden_state, adapter_down_weight, preferred_element_type=jnp.float32
    ).astype(jnp.bfloat16)
    backward_gradient = contract_axes(flattened_query, adapter_up_weight, 1, 1).astype(jnp.bfloat16)
    joined_terms = lax.psum_scatter(
        jnp.concatenate(
            [
                contract_axes(hidden_state, backward_gradient, 0, 0),
                contract_axes(flattened_query, adapter_latent, 0, 0),
            ],
            axis=1,
        ).astype(jnp.bfloat16),
        "seq",
        scatter_dimension=0,
        tiled=True,
    ).astype(jnp.float32)
    down_local = joined_terms[:, :adapter_rank_size]
    up_local = joined_terms[:, adapter_rank_size:]
    down_sum, up_sum = (
        lax.psum(down_local.astype(jnp.bfloat16), "dp").astype(jnp.float32),
        lax.psum(up_local.astype(jnp.bfloat16), "dp").astype(jnp.float32),
    )
    return (
        flattened_query.reshape(rollout_count, tokens, query_width),
        key_total,
        value_total,
        down_sum,
        up_sum.T,
    )


CHUNKS = 4
VMEM_BUDGET = 44 * 1024 * 1024
NEG = -1e30


def nt_dot(left, right):
    return lax.dot_general(
        left, right, (((1,), (1,)), ((), ())), preferred_element_type=jnp.float32
    )


def subsets(bits):
    masks = [0]
    for bit in bits:
        masks = masks + [mask | (1 << bit) for mask in masks]
    return masks


def fused_kernel(
    n_seq,
    n_dp,
    n_roll,
    tokens,
    kv_heads,
    group,
    rank,
    chunks,
    off_ref,
    len_ref,
    cos_ref,
    sin_ref,
    q_ref,
    k_ref,
    v_ref,
    g_ref,
    hid_ref,
    down_ref,
    up_ref,
    gq_ref,
    gk_ref,
    gv_ref,
    gd_ref,
    gu_ref,
    kv_all,
    dkv,
    red_buf,
    ad_buf,
    ad_red,
    dp_buf,
    ag_send,
    ag_recv,
    rs_send,
    rs_recv,
    ad_send,
    ad_recv,
    dp_send,
    dp_recv,
):
    me = lax.axis_index("seq")
    my_dp = lax.axis_index("dp")
    n_bits = n_seq.bit_length() - 1
    chip_bits = list(range(1, n_bits))
    gather_orders = [chip_bits + [0], chip_bits[::-1] + [0]]
    reduce_orders = [[0] + chip_bits[::-1], [0] + chip_bits]
    heads_per = kv_heads // chunks
    width = HEAD_WIDTH
    rows = group * tokens
    length = n_seq * tokens
    scale = width ** (-0.5)
    cols = q_ref.shape[1] // n_seq
    pending = []

    barrier = pltpu.get_barrier_semaphore()
    for bit in range(n_bits):
        pl.semaphore_signal(barrier, inc=1, device_id={"seq": me ^ (1 << bit)})
    for step in range(1, n_dp):
        pl.semaphore_signal(barrier, inc=1, device_id={"dp": lax.rem(my_dp + step, n_dp)})

    cos = cos_ref[...]
    sin = sin_ref[...]

    def slot_rows(mask):
        return pl.ds(pl.multiple_of((me ^ mask) * tokens, tokens), tokens)

    def load_chunk(c):
        for h in range(c * heads_per, (c + 1) * heads_per):
            for r in range(n_roll):
                span = slice(r * tokens, (r + 1) * tokens)
                lane = slice(h * width, (h + 1) * width)
                key = k_ref[span, lane].astype(jnp.float32)
                key = key * cos + pltpu.roll(key, width // 2, 1) * sin
                kv_all[0, h, r, slot_rows(0), :] = key.astype(jnp.bfloat16)
                kv_all[1, h, r, slot_rows(0), :] = v_ref[span, lane]

    gather_ops = {}

    def gather_send(c, stage):
        for t in range(2):
            order = gather_orders[t]
            bit = order[stage]
            for mask in subsets(order[:stage]):
                block = kv_all.at[
                    t, pl.ds(c * heads_per, heads_per), slice(None), slot_rows(mask), slice(None)
                ]
                got = mask | (1 << bit)
                copy = pltpu.make_async_remote_copy(
                    src_ref=block,
                    dst_ref=block,
                    send_sem=ag_send.at[t, c, got],
                    recv_sem=ag_recv.at[t, c, got],
                    device_id={"seq": me ^ (1 << bit)},
                )
                copy.start()
                gather_ops.setdefault((c, stage), []).append(copy)
                pending.append(copy)

    def gather_wait(c, stage):
        for copy in gather_ops[(c, stage)]:
            copy.wait_recv()

    reduce_ops = {}

    def reduce_send(c, stage):
        for t in range(2):
            order = reduce_orders[t]
            bit = order[stage]
            for rest in subsets(order[stage + 1 :]):
                mask = rest | (1 << bit)
                head_span = pl.ds(c * heads_per, heads_per)
                copy = pltpu.make_async_remote_copy(
                    src_ref=dkv.at[t, head_span, slice(None), slot_rows(mask), slice(None)],
                    dst_ref=red_buf.at[t, mask, head_span],
                    send_sem=rs_send.at[t, c, mask],
                    recv_sem=rs_recv.at[t, c, mask],
                    device_id={"seq": me ^ (1 << bit)},
                )
                copy.start()
                reduce_ops.setdefault((c, stage), []).append((t, mask, rest, copy))
                pending.append(copy)

    def reduce_add(c, stage):
        for t, mask, rest, copy in reduce_ops[(c, stage)]:
            copy.wait_recv()
            for h in range(c * heads_per, (c + 1) * heads_per):
                for r in range(n_roll):
                    total = dkv[t, h, r, slot_rows(rest), :].astype(jnp.float32)
                    total = total + red_buf[t, mask, h, r].astype(jnp.float32)
                    if stage < n_bits - 1:
                        dkv[t, h, r, slot_rows(rest), :] = total.astype(jnp.bfloat16)
                        continue
                    span = slice(r * tokens, (r + 1) * tokens)
                    lane = slice(h * width, (h + 1) * width)
                    if t == 0:
                        total = total * cos - pltpu.roll(total, width // 2, 1) * sin
                        gk_ref[span, lane] = total.astype(jnp.bfloat16)
                    else:
                        gv_ref[span, lane] = total.astype(jnp.bfloat16)

    def advance_reduce(c, stage):
        if stage > 0:
            reduce_add(c, stage - 1)
        if stage < n_bits:
            reduce_send(c, stage)

    adapter_ops = {}

    def adapter_send(stage):
        for t in range(2):
            order = reduce_orders[t]
            bit = order[stage]
            for rest in subsets(order[stage + 1 :]):
                mask = rest | (1 << bit)
                copy = pltpu.make_async_remote_copy(
                    src_ref=ad_buf.at[t, me ^ mask],
                    dst_ref=ad_red.at[t, mask],
                    send_sem=ad_send.at[t, mask],
                    recv_sem=ad_recv.at[t, mask],
                    device_id={"seq": me ^ (1 << bit)},
                )
                copy.start()
                adapter_ops.setdefault(stage, []).append((t, mask, rest, copy))
                pending.append(copy)

    def adapter_add(stage):
        for t, mask, rest, copy in adapter_ops[stage]:
            copy.wait_recv()
            total = ad_buf[t, me ^ rest].astype(jnp.float32) + ad_red[t, mask].astype(jnp.float32)
            total = total.astype(jnp.bfloat16)
            if stage < n_bits - 1:
                ad_buf[t, me ^ rest] = total
            else:
                dp_buf[my_dp, t] = total

    def advance_adapter(stage):
        if stage > 0:
            adapter_add(stage - 1)
        if stage < n_bits:
            adapter_send(stage)

    key_index = lax.broadcasted_iota(jnp.int32, (length, rows), 0)
    row_index = me * tokens + lax.broadcasted_iota(jnp.int32, (1, rows), 1) % tokens
    token_index = me * tokens + lax.broadcasted_iota(jnp.int32, (tokens, width), 0)

    def pair_work(c, index):
        h = c * heads_per + index // n_roll
        r = index % n_roll
        span = pl.ds(pl.multiple_of(r * tokens, tokens), tokens)
        offset = off_ref[r]
        keep = (token_index >= offset) & (token_index < len_ref[r])
        queries = []
        grads = []
        for j in range(group):
            lane = pl.ds(pl.multiple_of((h * group + j) * width, width), width)
            query = q_ref[span, lane].astype(jnp.float32)
            query = query * cos + pltpu.roll(query, width // 2, 1) * sin
            queries.append(query.astype(jnp.bfloat16))
            grad = g_ref[span, lane].astype(jnp.float32)
            grads.append(jnp.where(keep, grad, 0.0).astype(jnp.bfloat16))
        query = jnp.concatenate(queries, axis=0)
        grad = jnp.concatenate(grads, axis=0)
        key = kv_all[0, h, r]
        value = kv_all[1, h, r]
        visible = (key_index == row_index) | ((key_index >= offset) & (key_index <= row_index))
        scores = jnp.where(visible, nt_dot(key, query) * scale, NEG)
        weights = jnp.exp(scores - jnp.max(scores, axis=0, keepdims=True))
        prob = weights * (1.0 / jnp.sum(weights, axis=0, keepdims=True))
        grad_prob = nt_dot(value, grad)
        delta = jnp.sum(prob * grad_prob, axis=0, keepdims=True)
        grad_score = (prob * (grad_prob - delta) * scale).astype(jnp.bfloat16)
        prob_low = prob.astype(jnp.bfloat16)
        dkv[1, h, r] = jnp.dot(prob_low, grad, preferred_element_type=jnp.float32).astype(
            jnp.bfloat16
        )
        dkv[0, h, r] = jnp.dot(grad_score, query, preferred_element_type=jnp.float32).astype(
            jnp.bfloat16
        )
        back = jnp.dot(key.T, grad_score, preferred_element_type=jnp.float32).T
        for j in range(group):
            lane = pl.ds(pl.multiple_of((h * group + j) * width, width), width)
            part = back[j * tokens : (j + 1) * tokens]
            part = part * cos - pltpu.roll(part, width // 2, 1) * sin
            gq_ref[span, lane] = part.astype(jnp.bfloat16)

    def compute_chunk(c):
        def body(index, carry):
            pair_work(c, index)
            return carry

        lax.fori_loop(0, heads_per * n_roll, body, 0)

    load_chunk(0)
    pl.semaphore_wait(barrier, n_bits + n_dp - 1)
    latent = None
    for slot in range(chunks + 2 * n_bits + 1):
        for c in range(chunks):
            stage = slot - c
            if stage == 0 and c > 0:
                load_chunk(c)
            if 0 < stage <= n_bits:
                gather_wait(c, stage - 1)
            if 0 <= stage < n_bits:
                gather_send(c, stage)
        for c in range(chunks):
            stage = slot - c - n_bits
            if 1 <= stage <= n_bits:
                advance_reduce(c, stage)
        if slot == 0:
            latent = nt_dot(down_ref[...], hid_ref[...]).astype(jnp.bfloat16)
        ready = slot - n_bits
        if 0 <= ready < chunks:
            compute_chunk(ready)
            advance_reduce(ready, 0)
        if ready == chunks - 1:
            back = nt_dot(up_ref[...], gq_ref[...]).astype(jnp.bfloat16)
            for d in range(n_seq):
                lane = slice(d * cols, (d + 1) * cols)
                ad_buf[0, d] = jnp.dot(
                    back, hid_ref[:, lane], preferred_element_type=jnp.float32
                ).astype(jnp.bfloat16)
                ad_buf[1, d] = jnp.dot(
                    latent, gq_ref[:, lane], preferred_element_type=jnp.float32
                ).astype(jnp.bfloat16)
            advance_adapter(0)
        elif chunks <= ready < chunks + n_bits:
            advance_adapter(ready - chunks + 1)

    dp_ops = []
    for step in range(1, n_dp):
        copy = pltpu.make_async_remote_copy(
            src_ref=dp_buf.at[my_dp],
            dst_ref=dp_buf.at[my_dp],
            send_sem=dp_send.at[step],
            recv_sem=dp_recv.at[step],
            device_id={"dp": lax.rem(my_dp + step, n_dp)},
        )
        copy.start()
        dp_ops.append(copy)
        pending.append(copy)
    for copy in dp_ops:
        copy.wait_recv()
    down_total = dp_buf[0, 0].astype(jnp.float32)
    up_total = dp_buf[0, 1].astype(jnp.float32)
    for d in range(1, n_dp):
        down_total = down_total + dp_buf[d, 0].astype(jnp.float32)
        up_total = up_total + dp_buf[d, 1].astype(jnp.float32)
    gd_ref[...] = down_total
    gu_ref[...] = up_total
    for copy in pending:
        copy.wait_send()


def fused_on_device(
    n_seq,
    n_dp,
    queries,
    unrotated_key_rows,
    value_projection_rows,
    attention_output_gradient,
    normed_hidden_input,
    adapter_down_weight,
    adapter_up_weight,
    lengths,
    offsets,
):
    n_roll, tokens, q_width = queries.shape
    kv_width = unrotated_key_rows.shape[2]
    kv_heads = kv_width // HEAD_WIDTH
    group = q_width // kv_width
    rank = adapter_down_weight.shape[1]
    chunks = min(CHUNKS, kv_heads)
    flat = n_roll * tokens
    half = HEAD_WIDTH // 2
    frequency = rotary_base ** (-(jnp.arange(half, dtype=jnp.float32) * 2.0 / HEAD_WIDTH))
    positions = lax.axis_index("seq") * tokens + jnp.arange(tokens, dtype=jnp.int32)
    angles = positions.astype(jnp.float32)[:, None] * frequency[None, :]
    cosine, sine = jnp.cos(angles), jnp.sin(angles)
    cos_wide = jnp.concatenate([cosine, cosine], axis=1)
    sin_wide = jnp.concatenate([-sine, sine], axis=1)
    vmem = pl.BlockSpec(memory_space=pltpu.VMEM)
    smem = pl.BlockSpec(memory_space=pltpu.SMEM)
    cols = q_width // n_seq
    low = jnp.bfloat16
    dma = pltpu.SemaphoreType.DMA
    outs = pl.pallas_call(
        partial(fused_kernel, n_seq, n_dp, n_roll, tokens, kv_heads, group, rank, chunks),
        out_shape=(
            jax.ShapeDtypeStruct((flat, q_width), low),
            jax.ShapeDtypeStruct((flat, kv_width), low),
            jax.ShapeDtypeStruct((flat, kv_width), low),
            jax.ShapeDtypeStruct((rank, cols), jnp.float32),
            jax.ShapeDtypeStruct((rank, cols), jnp.float32),
        ),
        in_specs=[smem, smem] + [vmem] * 9,
        out_specs=[vmem] * 5,
        scratch_shapes=[
            pltpu.VMEM((2, kv_heads, n_roll, n_seq * tokens, HEAD_WIDTH), low),
            pltpu.VMEM((2, kv_heads, n_roll, n_seq * tokens, HEAD_WIDTH), low),
            pltpu.VMEM((2, n_seq, kv_heads, n_roll, tokens, HEAD_WIDTH), low),
            pltpu.VMEM((2, n_seq, rank, cols), low),
            pltpu.VMEM((2, n_seq, rank, cols), low),
            pltpu.VMEM((n_dp, 2, rank, cols), low),
            dma((2, chunks, n_seq)),
            dma((2, chunks, n_seq)),
            dma((2, chunks, n_seq)),
            dma((2, chunks, n_seq)),
            dma((2, n_seq)),
            dma((2, n_seq)),
            dma((n_dp,)),
            dma((n_dp,)),
        ],
        compiler_params=pltpu.CompilerParams(
            collective_id=0, has_side_effects=True, vmem_limit_bytes=60 * 1024 * 1024
        ),
    )(
        offsets,
        lengths,
        cos_wide,
        sin_wide,
        queries.reshape(flat, q_width),
        unrotated_key_rows.reshape(flat, kv_width),
        value_projection_rows.reshape(flat, kv_width),
        attention_output_gradient.reshape(flat, q_width),
        normed_hidden_input.reshape(flat, q_width),
        adapter_down_weight.T,
        adapter_up_weight,
    )
    grad_query, grad_key, grad_value, grad_down, grad_up = outs
    return (
        grad_query.reshape(n_roll, tokens, q_width),
        grad_key.reshape(n_roll, tokens, kv_width),
        grad_value.reshape(n_roll, tokens, kv_width),
        grad_down.T,
        grad_up,
    )


def dispatch(mesh, *args):
    n_seq = mesh.shape["seq"]
    n_roll, tokens, q_width = args[0].shape
    kv_width = args[1].shape[2]
    gathered = 2 * n_roll * n_seq * tokens * kv_width * 2
    if 3 * gathered + 7 * n_roll * tokens * q_width * 2 > VMEM_BUDGET:
        return on_device(*args)
    return fused_on_device(n_seq, mesh.shape["dp"], *args)


def solution(mesh):
    in_specs = (
        P("dp", "seq", None),
        P("dp", "seq", None),
        P("dp", "seq", None),
        P("dp", "seq", None),
        P("dp", "seq", None),
        P(),
        P(),
        P("dp"),
        P("dp"),
    )
    out_specs = (
        P("dp", "seq", None),
        P("dp", "seq", None),
        P("dp", "seq", None),
        P("seq", None),
        P(None, "seq"),
    )
    return jax.shard_map(
        partial(dispatch, mesh), mesh=mesh, in_specs=in_specs, out_specs=out_specs, check_vma=False
    )
```
